32 devices in a mesh: beam: 2 (over y), tm: 4 (over z), sect: 2 (over x), pol: 2 (over core).
Axes of the slice: x: 2, y: 2, z: 4, core: 2. Of those that a mesh axis runs over, the one named last changes fastest.
Arguments:
- signal: float32 [2, 2, 512, 4096], P(None, 'pol', ('beam', 'tm', 'sect')), parts along dimension 2, may hold values from -6 to 6
- coarse_taps: float32 [16, 4096], replicated, may hold values from -1.5 to 1.5
- fine_taps: float32 [16, 1024], replicated, may hold values from -1.5 to 1.5
- channel_order: int32 [4096], replicated, may hold values from 0 to 4095, each once
Outputs:
- fine_spectra: float32 [2, 2, 8192, 1, 1024], P(None, 'pol', ('beam', 'tm', 'sect')), parts along dimension 2
The draws below stay inside these ranges and needn't reach their ends.
There are 2 independent parts, one for each index of `beam`. The reference program is written for one: setup_inputs(seed, part) draws one part's arguments, and reference() takes and returns one part's arrays. A program takes and returns all parts, laid end to end along the dimension named above; an argument that names none is the same for every part. Nothing has to cross between parts.
Inputs may be any that keep to these rules, and one draw needn't show every extreme that they name: `channel_order`: each of the 4096 coarse channels appears exactly once.
All inputs are finite; a program needn't handle non-finite values.
Results may differ from the reference program's by a relative error of at most 0.0001.
Values sent between devices are 32-bit elements; how exact they have to be, the bound alone decides.
No kernel may reach another device: no remote copies, remote signals or barrier semaphores. Data moves between devices by JAX's collectives and lax.ppermute only.
A program may use at most 128 MiB of HBM per device.

```python
import jax
import jax.numpy as jnp
from jax import lax

COARSE = 4096
FINE = 1024
TAPS = 16
POL = 2
TSPEC = 256
FSPEC = 1


def block_scale(stream_key, shape, split, least, high):
    factor_of, own = 1.0, jax.random.fold_in(stream_key, 6)
    for position, parts in split:
        steps = jnp.exp(jax.random.uniform(jax.random.fold_in(own, position), (parts,), jnp.float32, least / len(split), high / len(split)))
        factor_of = factor_of * jnp.repeat(steps, shape[position] // parts).reshape([-1 if axis == position else 1 for axis in range(len(shape))])
    return factor_of


def gaussian(own_key, extent, width, reach, split=(), kind=jnp.bfloat16):
    gain = block_scale(own_key, extent, split, -0.22, 0.18) if split else 1.0
    result = jax.random.normal(own_key, extent, jnp.float32) * width * gain
    return jnp.minimum(jnp.maximum(result, -reach), reach).astype(kind)


def setup_inputs(seed: int = 0, part: int = 0) -> dict:
    key_of = jax.random.split(jax.random.key(seed), 5)
    part_keys = jax.random.split(jax.random.fold_in(key_of[4], part), 5)
    signal = gaussian(part_keys[0], (2, POL, TSPEC, COARSE), 1.0, 6.0, ((1, 2), (2, 8)), jnp.float32)
    coarse_taps = gaussian(key_of[1], (TAPS, COARSE), TAPS ** -0.5, 1.5, (), jnp.float32)
    fine_taps = gaussian(key_of[2], (TAPS, FINE), TAPS ** -0.5, 1.5, (), jnp.float32)
    channel_order = jax.random.permutation(key_of[3], COARSE).astype(jnp.int32)
    return dict(signal=signal, coarse_taps=coarse_taps, fine_taps=fine_taps, channel_order=channel_order)


def reference(signal, coarse_taps, fine_taps, channel_order):
    frame_count = TSPEC
    results = []
    for polar_index in range(signal.shape[1]):
        complex_slab = lax.complex(signal[0, polar_index], signal[1, polar_index])
        padded = jnp.concatenate([complex_slab, jnp.zeros((TAPS - 1, COARSE), complex_slab.dtype)], axis=0)
        filtered = coarse_taps[0] * padded[0:frame_count]
        for tap_index in range(1, TAPS):
            filtered = filtered + coarse_taps[tap_index] * padded[tap_index:tap_index + frame_count]
        coarse = jnp.fft.fft(filtered, axis=1, norm="ortho")
        series = jnp.take(coarse, channel_order, axis=1).T
        total_len = (FSPEC + TAPS - 1) * FINE
        series = jnp.pad(series, ((0, 0), (0, total_len - frame_count)))
        frames = series.reshape(COARSE, FSPEC + TAPS - 1, FINE)
        fine_filtered = fine_taps[0] * frames[:, 0:FSPEC]
        for tap_index in range(1, TAPS):
            fine_filtered = fine_filtered + fine_taps[tap_index] * frames[:, tap_index:tap_index + FSPEC]
        fine = jnp.fft.fft(fine_filtered, axis=2, norm="ortho")
        results.append(jnp.stack([jnp.real(fine), jnp.imag(fine)]))
    return jnp.stack(results, axis=1).astype(jnp.float32)
```

```python
from functools import partial
import math

import jax
import jax.numpy as jnp
import numpy as np
from jax import lax
from jax.sharding import PartitionSpec as P


def shifted(value, axis, steps):
    count = lax.axis_size(axis)
    initial, last = (max(0, -steps), min(count, count - steps))
    return lax.ppermute(value, axis, [(source, source + steps) for source in range(initial, last)])


def phase_table(rows, cols, period):
    product_mod = (
        lax.broadcasted_iota(jnp.int32, (rows, cols), 0)
        * lax.broadcasted_iota(jnp.int32, (rows, cols), 1)
        % period
    )
    angles = product_mod.astype(jnp.float32) * (-2.0 * math.pi / period)
    return (jnp.cos(angles), jnp.sin(angles))


def complex_einsum(form, left_re, left_im, right_re, right_im):
    product = partial(jnp.einsum, form, precision=lax.Precision.HIGH)
    return (
        product(left_re, right_re) - product(left_im, right_im),
        product(left_re, right_im) + product(left_im, right_re),
    )


def fine_table(rows, width):
    samples = np.arange(rows)[:, None] * np.arange(width)[None, :] % width
    angles = samples * (-2.0 * np.pi / width)
    return np.cos(angles).astype(np.float32), np.sin(angles).astype(np.float32)


def fine_bank(fine_taps, series):
    total_len = series.shape[3]
    tap_count, fine_width = fine_taps.shape
    frames = -(-total_len // fine_width)
    length = min(total_len, fine_width)
    padded = jnp.pad(series, ((0, 0), (0, 0), (0, 0), (0, frames * length - total_len)))
    blocks = padded.reshape(*series.shape[:3], frames, length)
    rows = []
    for frame in range(frames):
        row = fine_taps[0, :length] * blocks[:, :, :, frame]
        for tap_index in range(1, min(tap_count, frames - frame)):
            row = row + fine_taps[tap_index, :length] * blocks[:, :, :, frame + tap_index]
        rows.append(row)
    filtered = jnp.stack(rows, axis=3) * (1.0 / math.sqrt(fine_width))
    table_re, table_im = fine_table(length, fine_width)
    out_re, out_im = complex_einsum("pnfj,jm->pnfm", filtered[0], filtered[1], table_re, table_im)
    return jnp.stack([out_re, out_im])


def owner_bank(fine_taps, arrived):
    series = jnp.swapaxes(arrived[:, :, :, 0, :], 2, 3)
    return fine_bank(fine_taps, series)


def body(signal, coarse_taps, fine_taps, channel_order):
    polars = signal.shape[1]
    slab_len = signal.shape[2]
    coarse_width = signal.shape[3]
    tap_count = coarse_taps.shape[0]
    lead_rows = signal[:, :, : tap_count - 1, :]
    next_rows = shifted(lead_rows, ("tm", "sect"), -1)
    extended = jnp.concatenate([signal, next_rows], axis=2)
    filtered = coarse_taps[0] * extended[:, :, 0:slab_len, :]
    for tap_index in range(1, tap_count):
        filtered = (
            filtered + coarse_taps[tap_index] * extended[:, :, tap_index : tap_index + slab_len, :]
        )
    factor = math.isqrt(coarse_width)
    shaped = filtered.reshape(2, polars, slab_len, factor, factor)
    base_re, base_im = phase_table(factor, factor, factor)
    twist_re, twist_im = phase_table(factor, factor, coarse_width)
    section_re, section_im = complex_einsum("ptab,ak->ptkb", shaped[0], shaped[1], base_re, base_im)
    turned_re = section_re * twist_re - section_im * twist_im
    turned_im = section_re * twist_im + section_im * twist_re
    spec_re, spec_im = complex_einsum("ptkb,bm->ptmk", turned_re, turned_im, base_re, base_im)
    norm_scale = 1.0 / math.sqrt(coarse_width)
    spectra = jnp.stack([spec_re, spec_im]).reshape(2, polars, slab_len, coarse_width) * norm_scale
    ordered = jnp.take(spectra, channel_order, axis=3)
    owners = lax.axis_size(("tm", "sect"))
    own_count = coarse_width // owners
    blocks = ordered.reshape(2, polars, slab_len, owners, own_count)
    return owner_bank(
        fine_taps, lax.all_to_all(blocks, ("tm", "sect"), split_axis=3, concat_axis=2, tiled=True)
    )


def solution(mesh):
    in_specs = (P(None, "pol", ("beam", "tm", "sect"), None), P(), P(), P())
    out_specs = P(None, "pol", ("beam", "tm", "sect"), None, None)
    return jax.shard_map(body, mesh=mesh, in_specs=in_specs, out_specs=out_specs, check_vma=False)
```

```python
from functools import partial
import math

import jax
import jax.numpy as jnp
import numpy as np
from jax import lax
from jax.experimental import pallas as pl
from jax.experimental.pallas import tpu as pltpu
from jax.sharding import PartitionSpec as P

LANES = 128
ROWS = 8


def split(value):
    high = value.astype(jnp.bfloat16)
    return high, (value - high.astype(jnp.float32)).astype(jnp.bfloat16)


def host_split(value):
    high = value.astype(jnp.bfloat16)
    return high, (value - high.astype(np.float32)).astype(jnp.bfloat16)


def dft(rows, cols, period):
    angles = np.outer(np.arange(rows), np.arange(cols)) % period * (-2.0 * np.pi / period)
    return np.cos(angles), np.sin(angles)


def product3(left, right, dims):
    dot = partial(
        lax.dot_general, dimension_numbers=(dims, ((), ())), preferred_element_type=jnp.float32
    )
    return dot(left[0], right[0]) + (dot(left[0], right[1]) + dot(left[1], right[0]))


def coarse_tables(width):
    count = width // LANES
    re, im = dft(count, count, count)
    first = np.kron(np.block([[re, -im], [im, re]]), np.eye(ROWS)).astype(np.float32)
    twist = np.stack(dft(count, LANES, width)).astype(np.float32)
    re, im = dft(LANES, LANES, LANES)
    second = (np.concatenate([re, im], axis=1) / math.sqrt(width)).astype(np.float32)
    return (*host_split(first), twist, *host_split(second))


def coarse_kernel(
    index_ref, signal_ref, next_ref, taps_ref, first_hi, first_lo, twist_ref, second_hi, second_lo,
    out_ref, ext_ref, in_hi, in_lo, mid_hi, mid_lo, spec_ref,
):
    slab, width = signal_ref.shape[1:]
    lead = next_ref.shape[1]
    tap_count = taps_ref.shape[0]
    count = width // LANES
    groups = slab // ROWS
    for part in range(2):
        for a in range(count):
            cols = slice(a * LANES, (a + 1) * LANES)
            ext_ref[part, a, 0:slab] = signal_ref[part, :, cols]
            ext_ref[part, a, slab : slab + lead] = next_ref[part, :, cols]

    def filter_pair(pair, carry):
        tiles = []
        for half in range(2):
            a = 2 * pair + half
            taps = taps_ref[:, pl.ds(pl.multiple_of(a * LANES, LANES), LANES)]
            for part in range(2):
                for group in range(groups):
                    total = taps[0:1] * ext_ref[part, a, group * ROWS : (group + 1) * ROWS]
                    for k in range(1, tap_count):
                        start = group * ROWS + k
                        total = total + taps[k : k + 1] * ext_ref[part, a, start : start + ROWS]
                    tiles.append(total)
        for part in range(2):
            for group in range(groups):
                both = jnp.concatenate(
                    [tiles[part * groups + group], tiles[(2 + part) * groups + group]], axis=0
                )
                high, low = split(both)
                row = pl.multiple_of(part * count * ROWS + pair * 2 * ROWS, 2 * ROWS)
                in_hi[pl.ds(row, 2 * ROWS), group * LANES : (group + 1) * LANES] = high
                in_lo[pl.ds(row, 2 * ROWS), group * LANES : (group + 1) * LANES] = low
        return carry

    lax.fori_loop(0, count // 2, filter_pair, 0)

    inputs = (in_hi[...], in_lo[...])
    step = 8
    for chunk in range(count // step):
        rows = [
            slice((part * count + chunk * step) * ROWS, (part * count + (chunk + 1) * step) * ROWS)
            for part in range(2)
        ]
        re, im = [
            product3((first_hi[r, :], first_lo[r, :]), inputs, ((1,), (0,))) for r in rows
        ]
        twist_re = twist_ref[0, chunk * step : (chunk + 1) * step][:, None, :]
        twist_im = twist_ref[1, chunk * step : (chunk + 1) * step][:, None, :]
        turned_re, turned_im = [], []
        for group in range(groups):
            cols = slice(group * LANES, (group + 1) * LANES)
            sec_re = re[:, cols].reshape(step, ROWS, LANES)
            sec_im = im[:, cols].reshape(step, ROWS, LANES)
            turned_re.append(sec_re * twist_re - sec_im * twist_im)
            turned_im.append(sec_re * twist_im + sec_im * twist_re)
        turned_re = jnp.concatenate(turned_re, axis=1)
        turned_im = jnp.concatenate(turned_im, axis=1)
        upper = jnp.concatenate([turned_re, -turned_im], axis=2)
        lower = jnp.concatenate([turned_im, turned_re], axis=2)
        both = jnp.concatenate([upper, lower], axis=1).reshape(step * 2 * slab, 2 * LANES)
        high, low = split(both)
        mid_hi[chunk * step * 2 * slab : (chunk + 1) * step * 2 * slab, :] = high
        mid_lo[chunk * step * 2 * slab : (chunk + 1) * step * 2 * slab, :] = low

    pairs = count // 2
    for pair in range(pairs):
        rows = slice(pair * LANES, (pair + 1) * LANES)
        spec = product3(
            (second_hi[...], second_lo[...]), (mid_hi[rows, :], mid_lo[rows, :]), ((1,), (1,))
        )
        spec_ref[pair * LANES : (pair + 1) * LANES, :] = spec
        spec_ref[(pairs + pair) * LANES : (pairs + pair + 1) * LANES, :] = pltpu.roll(
            spec, LANES // 2, 1
        )

    total = out_ref.shape[0]
    left = lax.broadcasted_iota(jnp.int32, (1, LANES), 1) < LANES // 2

    def gather(block, carry):
        for row in range(ROWS):
            q = block * ROWS + row
            one = spec_ref[pl.ds(index_ref[q], 1), :]
            two = spec_ref[pl.ds(index_ref[total + q], 1), :]
            out_ref[pl.ds(q, 1), :] = jnp.where(left, one, two)
        return carry

    lax.fori_loop(0, total // ROWS, gather, 0)


def coarse_bank(signal, next_rows, taps, channel_order, owners):
    slab, width = signal.shape[1:]
    assert 4 * slab == LANES
    count = width // LANES
    own = width // owners
    order = channel_order.reshape(owners, 2, own // 2).swapaxes(0, 1)
    k, m = order % count, order // count
    flip = (k % 2) ^ jnp.arange(2, dtype=jnp.int32)[:, None, None]
    index = ((flip * (count // 2) + k // 2) * LANES + m).reshape(width)
    vmem = pl.BlockSpec(memory_space=pltpu.VMEM)
    size = 2 * count * ROWS
    groups = slab // ROWS
    return pl.pallas_call(
        coarse_kernel,
        out_shape=jax.ShapeDtypeStruct((width // 2, LANES), jnp.float32),
        in_specs=[pl.BlockSpec(memory_space=pltpu.SMEM)] + [vmem] * 8,
        out_specs=vmem,
        scratch_shapes=[
            pltpu.VMEM((2, count, slab + 16, LANES), jnp.float32),
            pltpu.VMEM((size, groups * LANES), jnp.bfloat16),
            pltpu.VMEM((size, groups * LANES), jnp.bfloat16),
            pltpu.VMEM((count * 2 * slab, 2 * LANES), jnp.bfloat16),
            pltpu.VMEM((count * 2 * slab, 2 * LANES), jnp.bfloat16),
            pltpu.VMEM((count * LANES, LANES), jnp.float32),
        ],
        name="coarse",
    )(index, signal, next_rows, taps, *coarse_tables(width))


def table_kernel(base_ref, turn_ref, high_ref, low_ref):
    length = base_ref.shape[1]
    width = high_ref.shape[1] // 2
    slab = 32
    for c in range(width // LANES):
        turn_re, turn_im = turn_ref[0, :, c : c + 1], turn_ref[1, :, c : c + 1]
        re = base_ref[0] * turn_re - base_ref[1] * turn_im
        im = base_ref[0] * turn_im + base_ref[1] * turn_re
        re, im = [value.reshape(length // slab, 1, slab, LANES) for value in (re, im)]
        for part, value in enumerate((jnp.concatenate([re, -im], 1), jnp.concatenate([im, re], 1))):
            high, low = split(value.reshape(2 * length, LANES))
            cols = slice(part * width + c * LANES, part * width + (c + 1) * LANES)
            high_ref[:, cols] = high
            low_ref[:, cols] = low


def fine_tables(length, width):
    base = np.stack(dft(length, LANES, width)).astype(np.float32)
    turn = np.stack(dft(length, width // LANES, width // LANES)).astype(np.float32)
    vmem = pl.BlockSpec(memory_space=pltpu.VMEM)
    shape = jax.ShapeDtypeStruct((2 * length, 2 * width), jnp.bfloat16)
    return pl.pallas_call(
        table_kernel, out_shape=(shape, shape), in_specs=[vmem] * 2, out_specs=(vmem, vmem),
        name="table",
    )(base, turn)


def fine_kernel(taps_ref, arrived_ref, high_ref, low_ref, out_ref):
    sources, pairs = arrived_ref.shape[:2]
    width = high_ref.shape[1] // 2
    count = width // LANES
    half = LANES // 2
    for side in range(2):
        x = jnp.concatenate(
            [arrived_ref[s, :, side * half : (side + 1) * half] for s in range(sources)], axis=1
        )
        x = split(x * taps_ref[...])
        for col in range(2 * count // 2):
            cols = slice(col * 2 * LANES, (col + 1) * 2 * LANES)
            y = product3(x, (high_ref[:, cols], low_ref[:, cols]), ((1,), (0,)))
            for sub in range(2):
                part, c = divmod(2 * col + sub, count)
                out_ref[part, side, pl.ds(c, pairs, stride=count), :] = y[
                    :, sub * LANES : (sub + 1) * LANES
                ]


def short_fine_bank(fine_taps, arrived, tables):
    sources, pairs = arrived.shape[:2]
    width = fine_taps.shape[1]
    slab = LANES // 4
    length = sources * slab
    taps = fine_taps[0, :length].reshape(sources, 1, slab) * (1.0 / math.sqrt(width))
    taps = jnp.broadcast_to(taps, (sources, 2, slab)).reshape(1, 2 * length)
    steps = 2
    block = pairs // steps
    count = width // LANES
    full = lambda shape: pl.BlockSpec(shape, lambda i: (0, 0))
    out = pl.pallas_call(
        fine_kernel,
        grid=(steps,),
        out_shape=jax.ShapeDtypeStruct((2, 2, pairs * count, LANES), jnp.float32),
        in_specs=[
            full((1, 2 * length)),
            pl.BlockSpec((sources, block, LANES), lambda i: (0, i, 0)),
            full((2 * length, 2 * width)),
            full((2 * length, 2 * width)),
        ],
        out_specs=pl.BlockSpec((2, 2, block * count, LANES), lambda i: (0, 0, i, 0)),
        name="fine",
    )(taps, arrived, *tables)
    return out.reshape(2, 1, 2 * pairs, 1, width)


def shifted(value, axis, steps):
    count = lax.axis_size(axis)
    initial, last = (max(0, -steps), min(count, count - steps))
    return lax.ppermute(value, axis, [(source, source + steps) for source in range(initial, last)])


def complex_einsum(form, left_re, left_im, right_re, right_im):
    product = partial(jnp.einsum, form, precision=lax.Precision.HIGH)
    return (
        product(left_re, right_re) - product(left_im, right_im),
        product(left_re, right_im) + product(left_im, right_re),
    )


def fine_table(rows, width):
    samples = np.arange(rows)[:, None] * np.arange(width)[None, :] % width
    angles = samples * (-2.0 * np.pi / width)
    return np.cos(angles).astype(np.float32), np.sin(angles).astype(np.float32)


def fine_bank(fine_taps, series):
    total_len = series.shape[3]
    tap_count, fine_width = fine_taps.shape
    frames = -(-total_len // fine_width)
    length = min(total_len, fine_width)
    padded = jnp.pad(series, ((0, 0), (0, 0), (0, 0), (0, frames * length - total_len)))
    blocks = padded.reshape(*series.shape[:3], frames, length)
    rows = []
    for frame in range(frames):
        row = fine_taps[0, :length] * blocks[:, :, :, frame]
        for tap_index in range(1, min(tap_count, frames - frame)):
            row = row + fine_taps[tap_index, :length] * blocks[:, :, :, frame + tap_index]
        rows.append(row)
    filtered = jnp.stack(rows, axis=3) * (1.0 / math.sqrt(fine_width))
    table_re, table_im = fine_table(length, fine_width)
    out_re, out_im = complex_einsum("pnfj,jm->pnfm", filtered[0], filtered[1], table_re, table_im)
    return jnp.stack([out_re, out_im])


def body(signal, coarse_taps, fine_taps, channel_order):
    slab_len, width = signal.shape[2:]
    tap_count = coarse_taps.shape[0]
    lead_rows = signal[:, 0, : tap_count - 1, :]
    next_rows = shifted(lead_rows, ("tm", "sect"), -1)
    owners = lax.axis_size(("tm", "sect"))
    own = width // owners
    length = owners * slab_len
    short = length <= fine_taps.shape[1]
    if short:
        tables = fine_tables(length, fine_taps.shape[1])
    ordered = coarse_bank(signal[:, 0], next_rows, coarse_taps, channel_order, owners)
    blocks = ordered.reshape(owners, own // 2, LANES)
    arrived = lax.all_to_all(blocks, ("tm", "sect"), split_axis=0, concat_axis=0, tiled=True)
    if short:
        return short_fine_bank(fine_taps, arrived, tables)
    series = arrived.reshape(owners, own // 2, 2, 2, slab_len).transpose(3, 2, 1, 0, 4)
    return fine_bank(fine_taps, series.reshape(2, 1, own, length))


def solution(mesh):
    in_specs = (P(None, "pol", ("beam", "tm", "sect"), None), P(), P(), P())
    out_specs = P(None, "pol", ("beam", "tm", "sect"), None, None)
    return jax.shard_map(body, mesh=mesh, in_specs=in_specs, out_specs=out_specs, check_vma=False)
```

```python
from functools import partial
import math

import jax
import jax.numpy as jnp
import numpy as np
from jax import lax
from jax.experimental import pallas as pl
from jax.experimental.pallas import tpu as pltpu
from jax.sharding import PartitionSpec as P


LANES = 128
ROWS = 8
HALF = 16
SIDES = LANES // (2 * HALF)


def split(value):
    high = value.astype(jnp.bfloat16)
    return high, (value - high.astype(jnp.float32)).astype(jnp.bfloat16)


def host_split(value):
    high = value.astype(jnp.bfloat16)
    return high, (value - high.astype(np.float32)).astype(jnp.bfloat16)


def dft(rows, cols, period):
    angles = np.outer(np.arange(rows), np.arange(cols)) % period * (-2.0 * np.pi / period)
    return np.cos(angles), np.sin(angles)


def product3(left, right, dims):
    dot = partial(
        lax.dot_general, dimension_numbers=(dims, ((), ())), preferred_element_type=jnp.float32
    )
    return dot(left[0], right[0]) + (dot(left[0], right[1]) + dot(left[1], right[0]))


def coarse_tables(width):
    count = width // LANES
    re, im = dft(count, count, count)
    first = np.kron(np.block([[re, -im], [im, re]]), np.eye(ROWS)).astype(np.float32)
    twist = np.stack(dft(count, LANES, width)).astype(np.float32)
    re, im = dft(LANES, LANES, LANES)
    second = (np.concatenate([re, im], axis=1) / math.sqrt(width)).astype(np.float32)
    return (*host_split(first), twist, *host_split(second))


def coarse_kernel(first, index_ref, signal_ref, *refs):
    *next_refs, taps_ref, first_hi, first_lo, twist_ref, second_hi, second_lo = refs[:-7]
    out_ref, ext_ref, in_hi, in_lo, mid_hi, mid_lo, spec_ref = refs[-7:]
    next_ref, start = (next_refs[0], 0) if next_refs else (signal_ref, first + HALF)
    slab, width = HALF, signal_ref.shape[2]
    tap_count = taps_ref.shape[0]
    lead = tap_count - 1
    count = width // LANES
    groups = slab // ROWS
    for part in range(2):
        for a in range(count):
            cols = slice(a * LANES, (a + 1) * LANES)
            ext_ref[part, a, 0:slab] = signal_ref[part, first : first + slab, cols]
            ext_ref[part, a, slab : slab + lead] = next_ref[part, start : start + lead, cols]

    def filter_pair(pair, carry):
        tiles = []
        for half in range(2):
            a = 2 * pair + half
            taps = taps_ref[:, pl.ds(pl.multiple_of(a * LANES, LANES), LANES)]
            for part in range(2):
                for group in range(groups):
                    total = taps[0:1] * ext_ref[part, a, group * ROWS : (group + 1) * ROWS]
                    for k in range(1, tap_count):
                        row = group * ROWS + k
                        total = total + taps[k : k + 1] * ext_ref[part, a, row : row + ROWS]
                    tiles.append(total)
        for part in range(2):
            for group in range(groups):
                both = jnp.concatenate(
                    [tiles[part * groups + group], tiles[(2 + part) * groups + group]], axis=0
                )
                high, low = split(both)
                row = pl.multiple_of(part * count * ROWS + pair * 2 * ROWS, 2 * ROWS)
                in_hi[pl.ds(row, 2 * ROWS), group * LANES : (group + 1) * LANES] = high
                in_lo[pl.ds(row, 2 * ROWS), group * LANES : (group + 1) * LANES] = low
        return carry

    lax.fori_loop(0, count // 2, filter_pair, 0)

    inputs = (in_hi[...], in_lo[...])
    step = 8
    for chunk in range(count // step):
        rows = [
            slice((part * count + chunk * step) * ROWS, (part * count + (chunk + 1) * step) * ROWS)
            for part in range(2)
        ]
        re, im = [
            product3((first_hi[r, :], first_lo[r, :]), inputs, ((1,), (0,))) for r in rows
        ]
        twist_re = twist_ref[0, chunk * step : (chunk + 1) * step][:, None, :]
        twist_im = twist_ref[1, chunk * step : (chunk + 1) * step][:, None, :]
        turned_re, turned_im = [], []
        for group in range(groups):
            cols = slice(group * LANES, (group + 1) * LANES)
            sec_re = re[:, cols].reshape(step, ROWS, LANES)
            sec_im = im[:, cols].reshape(step, ROWS, LANES)
            turned_re.append(sec_re * twist_re - sec_im * twist_im)
            turned_im.append(sec_re * twist_im + sec_im * twist_re)
        turned_re = jnp.concatenate(turned_re, axis=1)
        turned_im = jnp.concatenate(turned_im, axis=1)
        upper = jnp.concatenate([turned_re, -turned_im], axis=2)
        lower = jnp.concatenate([turned_im, turned_re], axis=2)
        both = jnp.concatenate([upper, lower], axis=1).reshape(step * 2 * slab, 2 * LANES)
        high, low = split(both)
        mid_hi[chunk * step * 2 * slab : (chunk + 1) * step * 2 * slab, :] = high
        mid_lo[chunk * step * 2 * slab : (chunk + 1) * step * 2 * slab, :] = low

    tiles = count // SIDES
    for tile in range(tiles // 2):
        rows = slice(tile * 2 * LANES, (tile + 1) * 2 * LANES)
        both = product3(
            (second_hi[...], second_lo[...]), (mid_hi[rows, :], mid_lo[rows, :]), ((1,), (1,))
        )
        for sub in range(2):
            spec = both[:, sub * LANES : (sub + 1) * LANES]
            for turn in range(SIDES):
                base = (turn * tiles + 2 * tile + sub) * LANES
                rolled = pltpu.roll(spec, turn * 2 * HALF, 1) if turn else spec
                spec_ref[base : base + LANES, :] = rolled

    total = out_ref.shape[0]
    lane = lax.broadcasted_iota(jnp.int32, (1, LANES), 1)

    def gather(block, carry):
        for row in range(ROWS):
            q = block * ROWS + row
            got = [spec_ref[pl.ds(index_ref[side * total + q], 1), :] for side in range(SIDES)]
            value = got[-1]
            for side in range(SIDES - 2, -1, -1):
                value = jnp.where(lane < (side + 1) * 2 * HALF, got[side], value)
            out_ref[pl.ds(q, 1), :] = value
        return carry

    lax.fori_loop(0, total // ROWS, gather, 0)


def slot_rows(channel_order, width, owners):
    count = width // LANES
    order = channel_order.reshape(owners, SIDES, width // owners // SIDES).swapaxes(0, 1)
    k, m = order % count, order // count
    turn = (jnp.arange(SIDES, dtype=jnp.int32)[:, None, None] - k % SIDES) % SIDES
    return ((turn * (count // SIDES) + k // SIDES) * LANES + m).reshape(width)


def coarse_bank(first, signals, taps, index):
    width = taps.shape[1]
    count = width // LANES
    vmem = pl.BlockSpec(memory_space=pltpu.VMEM)
    size = 2 * count * ROWS
    groups = HALF // ROWS
    return pl.pallas_call(
        partial(coarse_kernel, first),
        out_shape=jax.ShapeDtypeStruct((width // SIDES, LANES), jnp.float32),
        in_specs=[pl.BlockSpec(memory_space=pltpu.SMEM)] + [vmem] * (len(signals) + 6),
        out_specs=vmem,
        scratch_shapes=[
            pltpu.VMEM((2, count, HALF + 16, LANES), jnp.float32),
            pltpu.VMEM((size, groups * LANES), jnp.bfloat16),
            pltpu.VMEM((size, groups * LANES), jnp.bfloat16),
            pltpu.VMEM((count * 2 * HALF, 2 * LANES), jnp.bfloat16),
            pltpu.VMEM((count * 2 * HALF, 2 * LANES), jnp.bfloat16),
            pltpu.VMEM((count * LANES, LANES), jnp.float32),
        ],
    )(index, *signals, taps, *coarse_tables(width))


def table_kernel(base_ref, turn_ref, high_ref, low_ref):
    length = base_ref.shape[1]
    width = high_ref.shape[1] // 2
    slab = HALF
    for c in range(width // LANES):
        turn_re, turn_im = turn_ref[0, :, c : c + 1], turn_ref[1, :, c : c + 1]
        re = base_ref[0] * turn_re - base_ref[1] * turn_im
        im = base_ref[0] * turn_im + base_ref[1] * turn_re
        re, im = [value.reshape(length // slab, 1, slab, LANES) for value in (re, im)]
        for part, value in enumerate((jnp.concatenate([re, -im], 1), jnp.concatenate([im, re], 1))):
            high, low = split(value.reshape(2 * length, LANES))
            cols = slice(part * width + c * LANES, part * width + (c + 1) * LANES)
            high_ref[:, cols] = high
            low_ref[:, cols] = low


def by_half(value, axis, parts):
    shape = value.shape
    value = value.reshape(*shape[:axis], -1, parts, HALF, *shape[axis + 1 :])
    return value.swapaxes(axis, axis + 1).reshape(shape)


def fine_tables(length, width, parts):
    base = by_half(np.stack(dft(length, LANES, width)).astype(np.float32), 1, parts)
    turn = np.stack(dft(length, width // LANES, width // LANES)).astype(np.float32)
    turn = by_half(turn, 1, parts)
    vmem = pl.BlockSpec(memory_space=pltpu.VMEM)
    shape = jax.ShapeDtypeStruct((2 * length, 2 * width), jnp.bfloat16)
    return pl.pallas_call(
        table_kernel, out_shape=(shape, shape), in_specs=[vmem] * 2, out_specs=(vmem, vmem),
        name="table",
    )(base, turn)


def fine_kernel(taps_ref, *refs):
    *arrived, high_ref, low_ref, out_ref = refs
    sources, rows = arrived[0].shape[:2]
    width = high_ref.shape[1] // 2
    count = width // LANES
    piece = 2 * HALF
    x = jnp.concatenate(
        [
            jnp.concatenate(
                [
                    ref[s, :, side * piece : (side + 1) * piece]
                    for ref in arrived
                    for s in range(sources)
                ],
                axis=1,
            )
            for side in range(SIDES)
        ],
        axis=0,
    )
    x = split(x * taps_ref[...])
    for col in range(count):
        cols = slice(col * 2 * LANES, (col + 1) * 2 * LANES)
        y = product3(x, (high_ref[:, cols], low_ref[:, cols]), ((1,), (0,)))
        for sub in range(2):
            part, c = divmod(2 * col + sub, count)
            for side in range(SIDES):
                out_ref[part, side, pl.ds(c, rows, stride=count), :] = y[
                    side * rows : (side + 1) * rows, sub * LANES : (sub + 1) * LANES
                ]


def short_fine_bank(fine_taps, arrived, tables):
    parts = len(arrived)
    sources, own_rows = arrived[0].shape[:2]
    width = fine_taps.shape[1]
    length = parts * sources * HALF
    taps = by_half(fine_taps[0, :length] * (1.0 / math.sqrt(width)), 0, parts)
    taps = jnp.broadcast_to(taps.reshape(-1, 1, HALF), (parts * sources, 2, HALF))
    taps = taps.reshape(1, 2 * length)
    steps = 2
    block = own_rows // steps
    count = width // LANES
    full = lambda shape: pl.BlockSpec(shape, lambda i: (0, 0))
    out = pl.pallas_call(
        fine_kernel,
        grid=(steps,),
        out_shape=jax.ShapeDtypeStruct((2, SIDES, own_rows * count, LANES), jnp.float32),
        in_specs=[full((1, 2 * length))]
        + [pl.BlockSpec((sources, block, LANES), lambda i: (0, i, 0))] * parts
        + [full((2 * length, 2 * width))] * 2,
        out_specs=pl.BlockSpec((2, SIDES, block * count, LANES), lambda i: (0, 0, i, 0)),
        name="fine",
    )(taps, *arrived, *tables)
    return out.reshape(2, 1, SIDES * own_rows, 1, width)


def shifted(value, axis, steps):
    count = lax.axis_size(axis)
    initial, last = (max(0, -steps), min(count, count - steps))
    return lax.ppermute(value, axis, [(source, source + steps) for source in range(initial, last)])


def complex_einsum(form, left_re, left_im, right_re, right_im):
    product = partial(jnp.einsum, form, precision=lax.Precision.HIGH)
    return (
        product(left_re, right_re) - product(left_im, right_im),
        product(left_re, right_im) + product(left_im, right_re),
    )


def fine_table(rows, width):
    samples = np.arange(rows)[:, None] * np.arange(width)[None, :] % width
    angles = samples * (-2.0 * np.pi / width)
    return np.cos(angles).astype(np.float32), np.sin(angles).astype(np.float32)


def fine_bank(fine_taps, series):
    total_len = series.shape[3]
    tap_count, fine_width = fine_taps.shape
    frames = -(-total_len // fine_width)
    length = min(total_len, fine_width)
    padded = jnp.pad(series, ((0, 0), (0, 0), (0, 0), (0, frames * length - total_len)))
    blocks = padded.reshape(*series.shape[:3], frames, length)
    rows = []
    for frame in range(frames):
        row = fine_taps[0, :length] * blocks[:, :, :, frame]
        for tap_index in range(1, min(tap_count, frames - frame)):
            row = row + fine_taps[tap_index, :length] * blocks[:, :, :, frame + tap_index]
        rows.append(row)
    filtered = jnp.stack(rows, axis=3) * (1.0 / math.sqrt(fine_width))
    table_re, table_im = fine_table(length, fine_width)
    out_re, out_im = complex_einsum("pnfj,jm->pnfm", filtered[0], filtered[1], table_re, table_im)
    return jnp.stack([out_re, out_im])


def bank(signal, coarse_taps, fine_taps, channel_order):
    slab_len, width = signal.shape[2:]
    lead = coarse_taps.shape[0] - 1
    assert slab_len % HALF == 0 and lead <= HALF
    signal = signal[:, 0]
    next_rows = shifted(signal[:, :lead], ("tm", "sect"), -1)
    owners = lax.axis_size(("tm", "sect"))
    own = width // owners
    length = owners * slab_len
    parts = slab_len // HALF
    short = length <= fine_taps.shape[1]
    index = slot_rows(channel_order, width, owners)
    arrived = []
    for part in range(parts):
        first = part * HALF
        signals = [signal] if part < parts - 1 else [signal, next_rows]
        ordered = coarse_bank(first, signals, coarse_taps, index)
        blocks = ordered.reshape(owners, own // SIDES, LANES)
        arrived.append(
            lax.all_to_all(blocks, ("tm", "sect"), split_axis=0, concat_axis=0, tiled=True)
        )
    if short:
        tables = fine_tables(length, fine_taps.shape[1], parts)
        return short_fine_bank(fine_taps, arrived, tables)
    series = jnp.stack(arrived).reshape(parts, owners, own // SIDES, SIDES, 2, HALF)
    series = series.transpose(4, 3, 2, 1, 0, 5)
    return fine_bank(fine_taps, series.reshape(2, 1, own, length))


def solution(mesh):
    in_specs = (P(None, "pol", ("beam", "tm", "sect"), None), P(), P(), P())
    out_specs = P(None, "pol", ("beam", "tm", "sect"), None, None)
    return jax.shard_map(bank, mesh=mesh, in_specs=in_specs, out_specs=out_specs, check_vma=False)
```

```python
from functools import partial
import math

import jax
import jax.numpy as jnp
import numpy as np
from jax import lax
from jax.experimental import pallas as pl
from jax.experimental.pallas import tpu as pltpu
from jax.sharding import PartitionSpec as P


LANES = 128
ROWS = 8
HALF = 16
SIDES = LANES // (2 * HALF)


def split(value):
    high = value.astype(jnp.bfloat16)
    return high, (value - high.astype(jnp.float32)).astype(jnp.bfloat16)


def host_split(value):
    high = value.astype(jnp.bfloat16)
    return high, (value - high.astype(np.float32)).astype(jnp.bfloat16)


def dft(rows, cols, period):
    angles = np.outer(np.arange(rows), np.arange(cols)) % period * (-2.0 * np.pi / period)
    return np.cos(angles), np.sin(angles)


def product3(left, right, dims):
    dot = partial(
        lax.dot_general, dimension_numbers=(dims, ((), ())), preferred_element_type=jnp.float32
    )
    rows = left[0].shape[0]
    both = dot(jnp.concatenate(left, axis=0), right[0])
    return both[:rows] + (both[rows:] + dot(left[0], right[1]))


def coarse_tables(width):
    count = width // LANES
    re, im = dft(count, count, count)
    first = np.kron(np.block([[re, -im], [im, re]]), np.eye(ROWS)).astype(np.float32)
    twist = np.stack(dft(count, LANES, width)).astype(np.float32)
    re, im = dft(LANES, LANES, LANES)
    second = (np.concatenate([re, im], axis=1) / math.sqrt(width)).astype(np.float32)
    return (*host_split(first), twist, *host_split(second))


def coarse_kernel(first, index_ref, signal_ref, *refs):
    *next_refs, taps_ref, first_hi, first_lo, twist_ref, second_hi, second_lo = refs[:-7]
    out_ref, ext_ref, in_hi, in_lo, mid_hi, mid_lo, spec_ref = refs[-7:]
    next_ref, start = (next_refs[0], 0) if next_refs else (signal_ref, first + HALF)
    slab, width = HALF, signal_ref.shape[2]
    tap_count = taps_ref.shape[0]
    lead = tap_count - 1
    count = width // LANES
    groups = slab // ROWS
    for part in range(2):
        for a in range(count):
            cols = slice(a * LANES, (a + 1) * LANES)
            ext_ref[part, a, 0:slab] = signal_ref[part, first : first + slab, cols]
            ext_ref[part, a, slab : slab + lead] = next_ref[part, start : start + lead, cols]

    def filter_pair(pair, carry):
        tiles = []
        for half in range(2):
            a = 2 * pair + half
            taps = taps_ref[:, pl.ds(pl.multiple_of(a * LANES, LANES), LANES)]
            for part in range(2):
                for group in range(groups):
                    total = taps[0:1] * ext_ref[part, a, group * ROWS : (group + 1) * ROWS]
                    for k in range(1, tap_count):
                        row = group * ROWS + k
                        total = total + taps[k : k + 1] * ext_ref[part, a, row : row + ROWS]
                    tiles.append(total)
        for part in range(2):
            for group in range(groups):
                both = jnp.concatenate(
                    [tiles[part * groups + group], tiles[(2 + part) * groups + group]], axis=0
                )
                high, low = split(both)
                row = pl.multiple_of(part * count * ROWS + pair * 2 * ROWS, 2 * ROWS)
                in_hi[pl.ds(row, 2 * ROWS), group * LANES : (group + 1) * LANES] = high
                in_lo[pl.ds(row, 2 * ROWS), group * LANES : (group + 1) * LANES] = low
        return carry

    lax.fori_loop(0, count // 2, filter_pair, 0)

    inputs = (in_hi[...], in_lo[...])
    step = 8
    for chunk in range(count // step):
        rows = [
            slice((part * count + chunk * step) * ROWS, (part * count + (chunk + 1) * step) * ROWS)
            for part in range(2)
        ]
        re, im = [
            product3((first_hi[r, :], first_lo[r, :]), inputs, ((1,), (0,))) for r in rows
        ]
        twist_re = twist_ref[0, chunk * step : (chunk + 1) * step][:, None, :]
        twist_im = twist_ref[1, chunk * step : (chunk + 1) * step][:, None, :]
        turned_re, turned_im = [], []
        for group in range(groups):
            cols = slice(group * LANES, (group + 1) * LANES)
            sec_re = re[:, cols].reshape(step, ROWS, LANES)
            sec_im = im[:, cols].reshape(step, ROWS, LANES)
            turned_re.append(sec_re * twist_re - sec_im * twist_im)
            turned_im.append(sec_re * twist_im + sec_im * twist_re)
        turned_re = jnp.concatenate(turned_re, axis=1)
        turned_im = jnp.concatenate(turned_im, axis=1)
        upper = jnp.concatenate([turned_re, -turned_im], axis=2)
        lower = jnp.concatenate([turned_im, turned_re], axis=2)
        both = jnp.concatenate([upper, lower], axis=1).reshape(step * 2 * slab, 2 * LANES)
        high, low = split(both)
        mid_hi[chunk * step * 2 * slab : (chunk + 1) * step * 2 * slab, :] = high
        mid_lo[chunk * step * 2 * slab : (chunk + 1) * step * 2 * slab, :] = low

    tiles = count // SIDES
    for tile in range(tiles // 2):
        rows = slice(tile * 2 * LANES, (tile + 1) * 2 * LANES)
        both = product3(
            (second_hi[...], second_lo[...]), (mid_hi[rows, :], mid_lo[rows, :]), ((1,), (1,))
        )
        for sub in range(2):
            spec = both[:, sub * LANES : (sub + 1) * LANES]
            for turn in range(SIDES):
                base = (turn * tiles + 2 * tile + sub) * LANES
                rolled = pltpu.roll(spec, turn * 2 * HALF, 1) if turn else spec
                spec_ref[base : base + LANES, :] = rolled

    total = out_ref.shape[0]
    lane = lax.broadcasted_iota(jnp.int32, (1, LANES), 1)

    batch = math.gcd(total, 32)

    def gather(block, carry):
        values = []
        for row in range(batch):
            q = block * batch + row
            got = [spec_ref[pl.ds(index_ref[side * total + q], 1), :] for side in range(SIDES)]
            value = got[-1]
            for side in range(SIDES - 2, -1, -1):
                value = jnp.where(lane < (side + 1) * 2 * HALF, got[side], value)
            values.append(value)
        for tile in range(batch // ROWS):
            out_ref[pl.ds(pl.multiple_of(block * batch + tile * ROWS, ROWS), ROWS), :] = (
                jnp.concatenate(values[tile * ROWS : (tile + 1) * ROWS], axis=0)
            )
        return carry

    lax.fori_loop(0, total // batch, gather, 0)


def slot_rows(channel_order, width, owners):
    count = width // LANES
    order = channel_order.reshape(owners, SIDES, width // owners // SIDES).swapaxes(0, 1)
    k, m = order % count, order // count
    turn = (jnp.arange(SIDES, dtype=jnp.int32)[:, None, None] - k % SIDES) % SIDES
    return ((turn * (count // SIDES) + k // SIDES) * LANES + m).reshape(width)


def coarse_bank(first, signals, taps, index):
    width = taps.shape[1]
    count = width // LANES
    vmem = pl.BlockSpec(memory_space=pltpu.VMEM)
    size = 2 * count * ROWS
    groups = HALF // ROWS
    return pl.pallas_call(
        partial(coarse_kernel, first),
        out_shape=jax.ShapeDtypeStruct((width // SIDES, LANES), jnp.float32),
        in_specs=[pl.BlockSpec(memory_space=pltpu.SMEM)] + [vmem] * (len(signals) + 6),
        out_specs=vmem,
        scratch_shapes=[
            pltpu.VMEM((2, count, HALF + 16, LANES), jnp.float32),
            pltpu.VMEM((size, groups * LANES), jnp.bfloat16),
            pltpu.VMEM((size, groups * LANES), jnp.bfloat16),
            pltpu.VMEM((count * 2 * HALF, 2 * LANES), jnp.bfloat16),
            pltpu.VMEM((count * 2 * HALF, 2 * LANES), jnp.bfloat16),
            pltpu.VMEM((count * LANES, LANES), jnp.float32),
        ],
    )(index, *signals, taps, *coarse_tables(width))


def table_kernel(base_ref, turn_ref, high_ref, low_ref):
    length = base_ref.shape[1]
    width = high_ref.shape[1] // 2
    slab = HALF
    for c in range(width // LANES):
        turn_re, turn_im = turn_ref[0, :, c : c + 1], turn_ref[1, :, c : c + 1]
        re = base_ref[0] * turn_re - base_ref[1] * turn_im
        im = base_ref[0] * turn_im + base_ref[1] * turn_re
        re, im = [value.reshape(length // slab, 1, slab, LANES) for value in (re, im)]
        for part, value in enumerate((jnp.concatenate([re, -im], 1), jnp.concatenate([im, re], 1))):
            high, low = split(value.reshape(2 * length, LANES))
            cols = slice(part * width + c * LANES, part * width + (c + 1) * LANES)
            high_ref[:, cols] = high
            low_ref[:, cols] = low


def by_half(value, axis, parts):
    shape = value.shape
    value = value.reshape(*shape[:axis], -1, parts, HALF, *shape[axis + 1 :])
    return value.swapaxes(axis, axis + 1).reshape(shape)


def fine_tables(length, width, parts):
    base = by_half(np.stack(dft(length, LANES, width)).astype(np.float32), 1, parts)
    turn = np.stack(dft(length, width // LANES, width // LANES)).astype(np.float32)
    turn = by_half(turn, 1, parts)
    vmem = pl.BlockSpec(memory_space=pltpu.VMEM)
    shape = jax.ShapeDtypeStruct((2 * length, 2 * width), jnp.bfloat16)
    return pl.pallas_call(
        table_kernel, out_shape=(shape, shape), in_specs=[vmem] * 2, out_specs=(vmem, vmem),
        name="table",
    )(base, turn)


def fine_kernel(taps_ref, *refs):
    *arrived, high_ref, low_ref, out_ref = refs
    sources, rows = arrived[0].shape[:2]
    width = high_ref.shape[1] // 2
    count = width // LANES
    piece = 2 * HALF
    x = jnp.concatenate(
        [
            jnp.concatenate(
                [
                    ref[s, :, side * piece : (side + 1) * piece]
                    for ref in arrived
                    for s in range(sources)
                ],
                axis=1,
            )
            for side in range(SIDES)
        ],
        axis=0,
    )
    x = split(x * taps_ref[...])
    for col in range(count):
        cols = slice(col * 2 * LANES, (col + 1) * 2 * LANES)
        y = product3(x, (high_ref[:, cols], low_ref[:, cols]), ((1,), (0,)))
        for sub in range(2):
            part, c = divmod(2 * col + sub, count)
            for side in range(SIDES):
                out_ref[part, side, pl.ds(c, rows, stride=count), :] = y[
                    side * rows : (side + 1) * rows, sub * LANES : (sub + 1) * LANES
                ]


def short_fine_bank(fine_taps, arrived, tables):
    parts = len(arrived)
    sources, own_rows = arrived[0].shape[:2]
    width = fine_taps.shape[1]
    length = parts * sources * HALF
    taps = by_half(fine_taps[0, :length] * (1.0 / math.sqrt(width)), 0, parts)
    taps = jnp.broadcast_to(taps.reshape(-1, 1, HALF), (parts * sources, 2, HALF))
    taps = taps.reshape(1, 2 * length)
    steps = 2
    block = own_rows // steps
    count = width // LANES
    full = lambda shape: pl.BlockSpec(shape, lambda i: (0, 0))
    out = pl.pallas_call(
        fine_kernel,
        grid=(steps,),
        out_shape=jax.ShapeDtypeStruct((2, SIDES, own_rows * count, LANES), jnp.float32),
        in_specs=[full((1, 2 * length))]
        + [pl.BlockSpec((sources, block, LANES), lambda i: (0, i, 0))] * parts
        + [full((2 * length, 2 * width))] * 2,
        out_specs=pl.BlockSpec((2, SIDES, block * count, LANES), lambda i: (0, 0, i, 0)),
        name="fine",
    )(taps, *arrived, *tables)
    return out.reshape(2, 1, SIDES * own_rows, 1, width)


def shifted(value, axis, steps):
    count = lax.axis_size(axis)
    initial, last = (max(0, -steps), min(count, count - steps))
    return lax.ppermute(value, axis, [(source, source + steps) for source in range(initial, last)])


def complex_einsum(form, left_re, left_im, right_re, right_im):
    product = partial(jnp.einsum, form, precision=lax.Precision.HIGH)
    return (
        product(left_re, right_re) - product(left_im, right_im),
        product(left_re, right_im) + product(left_im, right_re),
    )


def fine_table(rows, width):
    samples = np.arange(rows)[:, None] * np.arange(width)[None, :] % width
    angles = samples * (-2.0 * np.pi / width)
    return np.cos(angles).astype(np.float32), np.sin(angles).astype(np.float32)


def fine_bank(fine_taps, series):
    total_len = series.shape[3]
    tap_count, fine_width = fine_taps.shape
    frames = -(-total_len // fine_width)
    length = min(total_len, fine_width)
    padded = jnp.pad(series, ((0, 0), (0, 0), (0, 0), (0, frames * length - total_len)))
    blocks = padded.reshape(*series.shape[:3], frames, length)
    rows = []
    for frame in range(frames):
        row = fine_taps[0, :length] * blocks[:, :, :, frame]
        for tap_index in range(1, min(tap_count, frames - frame)):
            row = row + fine_taps[tap_index, :length] * blocks[:, :, :, frame + tap_index]
        rows.append(row)
    filtered = jnp.stack(rows, axis=3) * (1.0 / math.sqrt(fine_width))
    table_re, table_im = fine_table(length, fine_width)
    out_re, out_im = complex_einsum("pnfj,jm->pnfm", filtered[0], filtered[1], table_re, table_im)
    return jnp.stack([out_re, out_im])


def bank(signal, coarse_taps, fine_taps, channel_order):
    slab_len, width = signal.shape[2:]
    lead = coarse_taps.shape[0] - 1
    assert slab_len % HALF == 0 and lead <= HALF
    signal = signal[:, 0]
    next_rows = shifted(signal[:, :lead], ("tm", "sect"), -1)
    owners = lax.axis_size(("tm", "sect"))
    own = width // owners
    length = owners * slab_len
    parts = slab_len // HALF
    short = length <= fine_taps.shape[1]
    index = slot_rows(channel_order, width, owners)
    arrived = []
    for part in range(parts):
        first = part * HALF
        signals = [signal] if part < parts - 1 else [signal, next_rows]
        ordered = coarse_bank(first, signals, coarse_taps, index)
        blocks = ordered.reshape(owners, own // SIDES, LANES)
        arrived.append(
            lax.all_to_all(blocks, ("tm", "sect"), split_axis=0, concat_axis=0, tiled=True)
        )
    if short:
        tables = fine_tables(length, fine_taps.shape[1], parts)
        return short_fine_bank(fine_taps, arrived, tables)
    series = jnp.stack(arrived).reshape(parts, owners, own // SIDES, SIDES, 2, HALF)
    series = series.transpose(4, 3, 2, 1, 0, 5)
    return fine_bank(fine_taps, series.reshape(2, 1, own, length))


def solution(mesh):
    in_specs = (P(None, "pol", ("beam", "tm", "sect"), None), P(), P(), P())
    out_specs = P(None, "pol", ("beam", "tm", "sect"), None, None)
    return jax.shard_map(bank, mesh=mesh, in_specs=in_specs, out_specs=out_specs, check_vma=False)
```
